32 devices in a mesh: row: 8 (over z, y), col: 4 (over x, core).
Axes of the slice: x: 2, y: 2, z: 4, core: 2. Of those that a mesh axis runs over, the one named last changes fastest.
Arguments:
- noise: float32 [8192, 512], P(('row', 'col')), may hold values from -40 to 40
- data: float32 [8192, 512], P(('col', 'row')), may hold values from -6 to 6
Outputs:
- noise_target: float32 [8192, 512], P(('row', 'col'))
- data_target: float32 [8192, 512], P(('col', 'row'))
- f_potential: float32 [8192], P('row')
- g_potential: float32 [8192], P('col')
The draws below stay inside these ranges and needn't reach their ends.
All inputs are finite; a program needn't handle non-finite values.
Results may differ from the reference program's by a relative error of at most 0.0003.
Values sent between devices are 32-bit elements; how exact they have to be, the bound alone decides.
A program may use at most 64 MiB of HBM per device.

```python
import jax
import jax.numpy as jnp
from jax import lax

W = 512
ITERS = 2
ROWS_DEV = 1024
COLS_DEV = 2048
NOISE = 8192
DATA = 8192


def draw_noise(key, part):
    base = jnp.clip(jax.random.normal(key, (NOISE, W), jnp.float32), -5.0, 5.0)
    return base


def block_scale(rng, shape, cuts, smallest, high):
    loudness, own = 1.0, jax.random.fold_in(rng, 6)
    for dim, blocks in cuts:
        draws = jnp.exp(jax.random.uniform(jax.random.fold_in(own, dim), (blocks,), jnp.float32, smallest / len(cuts), high / len(cuts)))
        loudness = loudness * jnp.repeat(draws, shape[dim] // blocks).reshape([-1 if axis == dim else 1 for axis in range(len(shape))])
    return loudness


def gaussian(stream_key, dims, deviation, limit, cuts=(), held_as=jnp.bfloat16):
    drawn = deviation * jax.random.normal(stream_key, dims, jnp.float32)
    if cuts:
        drawn = drawn * block_scale(stream_key, dims, cuts, -0.22, 0.18)
    return jnp.clip(drawn, -limit, limit).astype(held_as)


def setup_inputs(seed: int = 0) -> dict:
    arg_keys = jax.random.split(jax.random.key(seed), 3)
    return {
        "noise": draw_noise(jax.random.fold_in(arg_keys[2], 71), 0),
        "data": gaussian(arg_keys[1], (DATA, W), 1.0, 6.0, ((0, 32),), jnp.float32),
    }


EPSILON = 32.0


def costs(xb, yb):
    xn = jnp.sum(xb * xb, axis=1)
    yn = jnp.sum(yb * yb, axis=1)
    inner = jnp.dot(xb, yb.T, precision=lax.Precision.HIGHEST, preferred_element_type=jnp.float32)
    return xn[:, None] + yn[None, :] - 2.0 * inner


def row_pass(noise, data, g_now):
    blocks = noise.reshape(NOISE // ROWS_DEV, ROWS_DEV, W)

    def single(xb):
        scores = (g_now[None, :] - costs(xb, data)) / EPSILON
        peak = jnp.max(scores, axis=1)
        expo = jnp.exp(scores - peak[:, None])
        total = jnp.sum(expo, axis=1)
        f_part = -EPSILON * (peak + jnp.log(total))
        weights = expo / total[:, None]
        target = jnp.dot(weights, data, precision=lax.Precision.HIGHEST, preferred_element_type=jnp.float32)
        return f_part, target

    f_all, targets = lax.map(single, blocks)
    return f_all.reshape(NOISE), targets.reshape(NOISE, W)


def col_pass(noise, data, f_now):
    blocks = data.reshape(DATA // COLS_DEV, COLS_DEV, W)

    def single(yb):
        scores = (f_now[:, None] - costs(noise, yb)) / EPSILON
        peak = jnp.max(scores, axis=0)
        expo = jnp.exp(scores - peak[None, :])
        total = jnp.sum(expo, axis=0)
        g_part = -EPSILON * (peak + jnp.log(total))
        weights = expo / total[None, :]
        target = jnp.dot(weights.T, noise, precision=lax.Precision.HIGHEST, preferred_element_type=jnp.float32)
        return g_part, target

    g_all, targets = lax.map(single, blocks)
    return g_all.reshape(DATA), targets.reshape(DATA, W)


def reference(noise, data):
    g_now = jnp.zeros((DATA,), jnp.float32)
    f_now = jnp.zeros((NOISE,), jnp.float32)
    data_target = jnp.zeros((DATA, W), jnp.float32)
    for step in range(ITERS):
        f_now, unused = row_pass(noise, data, g_now)
        g_now, data_target = col_pass(noise, data, f_now)
    unused_f, noise_target = row_pass(noise, data, g_now)
    return noise_target, data_target, f_now, g_now
```

```python
import functools
import math

import jax
import jax.numpy as jnp
from jax import lax
from jax.experimental import pallas as pl
from jax.experimental.pallas import tpu as pltpu
from jax.sharding import PartitionSpec as P

MESH = pl.DeviceIdType.MESH
EPSILON = 32.0
UNIT = math.log2(math.e) / EPSILON
BACK = EPSILON * math.log(2.0)
SCALE = 2.0 * UNIT


def split(v):
    hi = v.astype(jnp.bfloat16)
    return hi, (v - hi.astype(jnp.float32)).astype(jnp.bfloat16)


def dot3(ah, al, bh, bl):
    d = functools.partial(jnp.dot, preferred_element_type=jnp.float32)
    return d(ah, bh) + (d(ah, bl) + d(al, bh))


def kernel(
    nr, nc,
    x_ref, y_ref,
    nt_ref, dt_ref, f_ref, g_ref,
    x_full, y_full, scores, xsh, xsl, xth, xtl, ysh, ysl, yth, ytl,
    eh, el, part, npart, pm, ps, fcol, xn, yn, gvec, cloc,
    rstat, cstat, rsbuf, first, nsbuf,
    ag_s, ag_r, x_s, x_r, rst_s, rst_r, cst_s, cst_r, rs_s, rs_r, ns_s, ns_r,
):
    row, col = lax.axis_index("row"), lax.axis_index("col")
    xb, w = x_ref.shape
    yb = y_ref.shape[0]
    rows, cols = scores.shape
    half, hw = yb // 2, w // 2

    def index_of(p):
        q = lax.div(p, nr // 2)
        return (1 - q) * (2 * p) + q * (2 * (nr - 1 - p) + 1)

    odd = lax.rem(row, 2)
    pos = (1 - odd) * lax.div(row, 2) + odd * (nr - 1 - lax.div(row, 2))

    def at(d):
        return index_of(lax.rem(pos + d + 2 * nr, nr))

    sides = (1, -1)
    barrier = pltpu.get_barrier_semaphore()
    for o in range(1, nr):
        pl.semaphore_signal(barrier, inc=1, device_id=(lax.rem(row + o, nr), col), device_id_type=MESH)
    for o in range(1, nc):
        pl.semaphore_signal(barrier, inc=1, device_id=(row, lax.rem(col + o, nc)), device_id_type=MESH)
    pl.semaphore_wait(barrier, nr + nc - 2)

    pending = []

    def send(src, dst, ss, rs, dev):
        c = pltpu.make_async_remote_copy(src_ref=src, dst_ref=dst, send_sem=ss, recv_sem=rs, device_id=dev, device_id_type=MESH)
        c.start()
        pending.append(c)

    def arrive(dst, ss, rs, dev):
        pltpu.make_async_remote_copy(src_ref=dst, dst_ref=dst, send_sem=ss, recv_sem=rs, device_id=dev, device_id_type=MESH).wait_recv()

    def piece(ref, o, d):
        return ref.at[o, pl.ds(d * half, half)]

    def ag_send(s):
        for d in range(2):
            o = at(-sides[d] * s)
            src = y_ref.at[pl.ds(d * half, half)] if s == 0 else piece(y_full, o, d)
            send(src, piece(y_full, o, d), ag_s.at[s, d], ag_r.at[s, d], (at(sides[d]), col))

    def ag_wait(s):
        for d in range(2):
            o = at(-sides[d] * (s + 1))
            arrive(piece(y_full, o, d), ag_s.at[s, d], ag_r.at[s, d], (at(sides[d]), col))

    def peers(n, me, ss, rs, src, dst, dev):
        for o in range(1, n):
            send(src, dst, ss.at[o], rs.at[me], dev(lax.rem(me + o, n)))

    def peers_wait(n, me, ss, rs, dst, dev):
        for o in range(1, n):
            k = lax.rem(me + o, n)
            arrive(dst(k), ss.at[o], rs.at[k], dev(k))

    in_col = lambda k: (row, k)
    in_row = lambda k: (k, col)

    ag_send(0)
    peers(nc, col, x_s, x_r, x_ref, x_full.at[col], in_col)
    x_full[col] = x_ref[...]
    y_full[row] = y_ref[...]

    def prep_x(k, _):
        r0 = pl.ds(pl.multiple_of(k * xb, xb), xb)
        v = x_full[k] * SCALE
        xsh[r0, :], xsl[r0, :] = split(v)
        t = v.T
        xth[:, r0], xtl[:, r0] = split(t)
        xn[:, r0] = jnp.sum(t * t, axis=0, keepdims=True) * (1.0 / (SCALE * SCALE))
        return 0

    tile = 256

    def block(o):
        c0 = pl.ds(pl.multiple_of(o * yb, yb), yb)
        v = y_full[o]
        ysh[c0, :], ysl[c0, :] = split(v)
        t = v.T
        yth[...], ytl[...] = split(t)
        yn[:, c0] = jnp.sum(t * t, axis=0, keepdims=True)

        def body(i, _):
            r0 = pl.ds(pl.multiple_of(i * tile, tile), tile)
            scores[r0, c0] = dot3(xsh[r0, :], xsl[r0, :], yth[...], ytl[...])
            return 0

        lax.fori_loop(0, rows // tile, body, 0)

    def blocks(d):
        lax.fori_loop(0, 2, lambda i, _: (block(at(d * (1 - 2 * i))), 0)[1], 0)

    for s in range(1, nr):
        ag_wait(s - 1)
        if s < nr - 1:
            ag_send(s)
        if s == nr // 2:
            peers_wait(nc, col, x_s, x_r, lambda k: x_full.at[k], in_col)
            lax.fori_loop(0, nc, prep_x, 0)
            lax.fori_loop(0, 2, lambda i, _: (block(at(i * s)), 0)[1], 0)
        elif s > nr // 2:
            blocks(s)

    rt = 32

    def row_pass(ph, keep):
        def body(i, _):
            r0 = pl.ds(pl.multiple_of(i * rt, rt), rt)
            top = scores[r0, 0:128] + gvec[:, 0:128]
            for c in range(128, cols, 128):
                top = jnp.maximum(top, scores[r0, c:c + 128] + gvec[:, c:c + 128])
            top = jnp.broadcast_to(jnp.max(top, axis=1, keepdims=True), (rt, 128))
            acc = jnp.zeros((rt, 128), jnp.float32)
            for c in range(0, cols, 128):
                e = jnp.exp2(scores[r0, c:c + 128] + gvec[:, c:c + 128] - top)
                acc = acc + e
                if keep:
                    eh[r0, c:c + 128], el[r0, c:c + 128] = split(e)
            pm[r0, :] = top
            ps[r0, :] = acc
            return 0

        lax.fori_loop(0, rows // rt, body, 0, unroll=2)
        rstat[ph, col, 0:1, :] = jnp.max(pm[...].T, axis=0, keepdims=True)
        rstat[ph, col, 1:2, :] = jnp.sum(ps[...].T, axis=0, keepdims=True)
        peers(nc, col, rst_s.at[ph], rst_r.at[ph], rstat.at[ph, col], rstat.at[ph, col], in_col)

    def merge(ref, n):
        peak = ref[0, 0:1, :]
        for k in range(1, n):
            peak = jnp.maximum(peak, ref[k, 0:1, :])
        total = ref[0, 1:2, :] * jnp.exp2(ref[0, 0:1, :] - peak)
        for k in range(1, n):
            total = total + ref[k, 1:2, :] * jnp.exp2(ref[k, 0:1, :] - peak)
        return peak, total

    def row_merge(ph):
        peers_wait(nc, col, rst_s.at[ph], rst_r.at[ph], lambda k: rstat.at[ph, k], in_col)
        return merge(rstat.at[ph], nc)

    def to_column(v):
        fcol[...] = jnp.broadcast_to(v, (128, rows)).T

    def col_pass(ph, keep):
        def body(i, _):
            c0 = pl.ds(pl.multiple_of(i * 128, 128), 128)
            a = scores[:, c0] + fcol[...]
            top = jnp.max(a, axis=0, keepdims=True)
            e = jnp.exp2(a - top)
            cstat[ph, row, 0:1, c0] = top
            cstat[ph, row, 1:2, c0] = jnp.sum(e, axis=0, keepdims=True)
            if keep:
                eh[:, c0], el[:, c0] = split(e)
            return 0

        lax.fori_loop(0, cols // 128, body, 0)
        peers(nr, row, cst_s.at[ph], cst_r.at[ph], cstat.at[ph, row], cstat.at[ph, row], in_row)

    def col_merge(ph):
        peers_wait(nr, row, cst_s.at[ph], cst_r.at[ph], lambda k: cstat.at[ph, k], in_row)
        return merge(cstat.at[ph], nr)

    gvec[...] = yn[...] * -UNIT
    for it in range(2):
        row_pass(it, False)
        peak, total = row_merge(it)
        f_new = -(peak + jnp.log2(total))
        if it == 1:
            f_ref[...] = f_new * BACK + xn[...]
        to_column(f_new)
        col_pass(it, it == 1)
        if it == 0:
            peak, total = col_merge(0)
            gvec[...] = -(peak + jnp.log2(total))

    def chunk(o):
        return pl.ds(pl.multiple_of(o * yb, yb), yb)

    def weigh(s, d):
        c0 = chunk(at(-sides[d] * (1 + s)))
        w0 = pl.ds(d * hw, hw)
        part[w0, c0] = dot3(xth[w0, :], xtl[w0, :], eh[:, c0], el[:, c0])

    def weigh_steps(lo, hi):
        def body(s, _):
            for d in range(2):
                weigh(s, d)
            return 0

        lax.fori_loop(lo, hi, body, 0)

    def mine(s, d):
        c0 = chunk(at(-sides[d] * (1 + s)))
        return part[pl.ds(d * hw, hw), c0] * cloc[:, c0]

    def rs_step(s):
        for d in range(2):
            if s == 0:
                first[d] = mine(0, d)
                src = first.at[d]
            else:
                src = rsbuf.at[s - 1, d]
                arrive(src, rs_s.at[s - 1, d], rs_r.at[s - 1, d], (at(sides[d]), col))
                rsbuf[s - 1, d] = rsbuf[s - 1, d] + mine(s, d)
            if s < nr - 1:
                send(src, rsbuf.at[s, d], rs_s.at[s, d], rs_r.at[s, d], (at(sides[d]), col))

    weigh_steps(0, nr // 2)
    peak, total = col_merge(1)
    cloc[...] = jnp.exp2(cstat[1, row, 0:1, :] - peak) / total * (1.0 / SCALE)
    rs_step(0)
    gvec[...] = -(peak + jnp.log2(total))
    g_ref[...] = gvec[...] * BACK + yn[...]
    weigh_steps(nr // 2, nr)
    rs_step(1)

    row_pass(2, True)
    rs_step(2)

    def spread(k):
        r0 = pl.ds(pl.multiple_of(k * xb, xb), xb)
        npart[r0, :] = dot3(eh[r0, :], el[r0, :], ysh[...], ysl[...])

    mid = max(1, nc // 2)
    lax.fori_loop(0, mid, lambda i, _: (spread(lax.rem(col + 1 + i, nc)), 0)[1], 0)
    peak, total = row_merge(2)
    to_column(jnp.exp2(rstat[2, col, 0:1, :] - peak) / total)

    def scaled(k):
        r0 = pl.ds(pl.multiple_of(k * xb, xb), xb)
        fc = fcol[r0, :]
        for c in range(0, w, 128):
            npart[r0, c:c + 128] = npart[r0, c:c + 128] * fc
        return r0

    def push(o):
        k = lax.rem(col + o, nc)
        r0 = scaled(k)
        send(npart.at[r0], nsbuf.at[col], ns_s.at[o], ns_r.at[col], in_col(k))

    for o in range(1, min(mid + 1, nc)):
        push(o)
    if nr > 4:
        rs_step(3)
    lax.fori_loop(mid, nc, lambda i, _: (spread(lax.rem(col + 1 + i, nc)), 0)[1], 0)
    for o in range(mid + 1, nc):
        push(o)
    nsbuf[col] = npart[scaled(col), :]
    for s in range(4 if nr > 4 else 3, nr):
        rs_step(s)
    for d in range(2):
        dt_ref[:, d * hw:(d + 1) * hw] = rsbuf[nr - 2, d].T
    peers_wait(nc, col, ns_s, ns_r, lambda k: nsbuf.at[k], in_col)
    acc = nsbuf[0]
    for k in range(1, nc):
        acc = acc + nsbuf[k]
    nt_ref[...] = acc
    for c in pending:
        c.wait_send()


def solution(mesh):
    nr, nc = mesh.shape["row"], mesh.shape["col"]

    def shards(noise, data):
        xb, w = noise.shape
        yb = data.shape[0]
        rows, cols = xb * nc, yb * nr
        f32, bf = jnp.float32, jnp.bfloat16
        vmem = pltpu.VMEM
        dma = pltpu.SemaphoreType.DMA
        out = pl.pallas_call(
            functools.partial(kernel, nr, nc),
            out_shape=(
                jax.ShapeDtypeStruct((xb, w), f32),
                jax.ShapeDtypeStruct((yb, w), f32),
                jax.ShapeDtypeStruct((1, rows), f32),
                jax.ShapeDtypeStruct((1, cols), f32),
            ),
            in_specs=[pl.BlockSpec(memory_space=pltpu.VMEM)] * 2,
            out_specs=(pl.BlockSpec(memory_space=pltpu.VMEM),) * 4,
            scratch_shapes=[
                vmem((nc, xb, w), f32), vmem((nr, yb, w), f32), vmem((rows, cols), f32),
                vmem((rows, w), bf), vmem((rows, w), bf), vmem((w, rows), bf), vmem((w, rows), bf),
                vmem((cols, w), bf), vmem((cols, w), bf), vmem((w, yb), bf), vmem((w, yb), bf),
                vmem((rows, cols), bf), vmem((rows, cols), bf), vmem((w, cols), f32), vmem((rows, w), f32),
                vmem((rows, 128), f32), vmem((rows, 128), f32), vmem((rows, 128), f32),
                vmem((1, rows), f32), vmem((1, cols), f32), vmem((1, cols), f32), vmem((1, cols), f32),
                vmem((3, nc, 2, rows), f32), vmem((2, nr, 2, cols), f32),
                vmem((nr - 1, 2, w // 2, yb), f32), vmem((2, w // 2, yb), f32), vmem((nc, xb, w), f32),
                dma((nr - 1, 2)), dma((nr - 1, 2)), dma((nc,)), dma((nc,)),
                dma((3, nc)), dma((3, nc)), dma((2, nr)), dma((2, nr)),
                dma((nr - 1, 2)), dma((nr - 1, 2)), dma((nc,)), dma((nc,)),
            ],
            compiler_params=pltpu.CompilerParams(
                collective_id=0, has_side_effects=True, vmem_limit_bytes=60 * 1024 * 1024
            ),
        )(noise, data)
        return out[0], out[1], out[2].reshape(rows), out[3].reshape(cols)

    return jax.shard_map(
        shards,
        mesh=mesh,
        in_specs=(P(("row", "col"), None), P(("col", "row"), None)),
        out_specs=(P(("row", "col"), None), P(("col", "row"), None), P("row"), P("col")),
        check_vma=False,
    )
```

```python
import functools
import math

import jax
import jax.numpy as jnp
from jax import lax
from jax.experimental import pallas as pl
from jax.experimental.pallas import tpu as pltpu
from jax.sharding import PartitionSpec as P

MESH = pl.DeviceIdType.MESH
EPSILON = 32.0
UNIT = math.log2(math.e) / EPSILON
BACK = EPSILON * math.log(2.0)
SCALE = 2.0 * UNIT
PIECES = 2
LOWEST = -3e38


def split(v):
    hi = v.astype(jnp.bfloat16)
    return hi, (v - hi.astype(jnp.float32)).astype(jnp.bfloat16)


def dot3(ah, al, bh, bl):
    d = functools.partial(jnp.dot, preferred_element_type=jnp.float32)
    return d(ah, bh) + (d(ah, bl) + d(al, bh))


def kernel(
    nr, nc,
    x_ref, y_ref,
    nt_ref, dt_ref, f_ref, g_ref,
    x_full, y_full, scores, xsh, xsl, xth, xtl, ysh, ysl, yth, ytl,
    eh, el, part, npart, pm, ps, fcol, xn, yn, gvec, cloc,
    rstat, cstat, rsbuf, first, nsbuf,
    ag_s, ag_r, x_s, x_r, rst_s, rst_r, cst_s, cst_r, rs_s, rs_r, ns_s, ns_r,
):
    row, col = lax.axis_index("row"), lax.axis_index("col")
    xb, w = x_ref.shape
    yb = y_ref.shape[0]
    rows, cols = scores.shape
    half, hw = yb // 2, w // 2
    hy, hq = half // PIECES, hw // PIECES

    def index_of(p):
        q = lax.div(p, nr // 2)
        return (1 - q) * (2 * p) + q * (2 * (nr - 1 - p) + 1)

    odd = lax.rem(row, 2)
    pos = (1 - odd) * lax.div(row, 2) + odd * (nr - 1 - lax.div(row, 2))

    def at(d):
        return index_of(lax.rem(pos + d + 2 * nr, nr))

    sides = (1, -1)
    barrier = pltpu.get_barrier_semaphore()
    for o in range(1, nr):
        pl.semaphore_signal(barrier, inc=1, device_id=(lax.rem(row + o, nr), col), device_id_type=MESH)
    for o in range(1, nc):
        pl.semaphore_signal(barrier, inc=1, device_id=(row, lax.rem(col + o, nc)), device_id_type=MESH)
    pl.semaphore_wait(barrier, nr + nc - 2)

    pending = []

    def send(src, dst, ss, rs, dev):
        c = pltpu.make_async_remote_copy(src_ref=src, dst_ref=dst, send_sem=ss, recv_sem=rs, device_id=dev, device_id_type=MESH)
        c.start()
        pending.append(c)

    def arrive(dst, ss, rs, dev):
        pltpu.make_async_remote_copy(src_ref=dst, dst_ref=dst, send_sem=ss, recv_sem=rs, device_id=dev, device_id_type=MESH).wait_recv()

    def piece(ref, o, d, q):
        return ref.at[o, pl.ds(d * half + q * hy, hy)]

    def ag_step(s):
        for q in range(PIECES):
            for d in range(2):
                o, dev = at(-sides[d] * s), (at(sides[d]), col)
                dst = piece(y_full, o, d, q)
                if s > 0:
                    arrive(dst, ag_s.at[s - 1, d, q], ag_r.at[s - 1, d, q], dev)
                if s < nr - 1:
                    src = y_ref.at[pl.ds(d * half + q * hy, hy)] if s == 0 else dst
                    send(src, dst, ag_s.at[s, d, q], ag_r.at[s, d, q], dev)

    def peers(n, me, ss, rs, src, dst, dev):
        for o in range(1, n):
            send(src, dst, ss.at[o], rs.at[me], dev(lax.rem(me + o, n)))

    def peers_wait(n, me, ss, rs, dst, dev):
        for o in range(1, n):
            k = lax.rem(me + o, n)
            arrive(dst(k), ss.at[o], rs.at[k], dev(k))

    in_col = lambda k: (row, k)
    in_row = lambda k: (k, col)

    ag_step(0)
    peers(nc, col, x_s, x_r, x_ref, x_full.at[col], in_col)
    x_full[col] = x_ref[...]
    pm[...] = jnp.full_like(pm, LOWEST)
    ps[...] = jnp.zeros_like(ps)
    y_full[row] = y_ref[...]

    def prep_x(k, _):
        r0 = pl.ds(pl.multiple_of(k * xb, xb), xb)
        v = x_full[k] * SCALE
        xsh[r0, :], xsl[r0, :] = split(v)
        t = v.T
        xth[:, r0], xtl[:, r0] = split(t)
        xn[:, r0] = jnp.sum(t * t, axis=0, keepdims=True) * (1.0 / (SCALE * SCALE))
        return 0

    tile = 256

    def block(o):
        c0 = pl.ds(pl.multiple_of(o * yb, yb), yb)
        v = y_full[o]
        ysh[c0, :], ysl[c0, :] = split(v)
        t = v.T
        yth[...], ytl[...] = split(t)
        norm = jnp.sum(t * t, axis=0, keepdims=True)
        yn[:, c0] = norm
        start = norm * -UNIT

        def body(i, _):
            r0 = pl.ds(pl.multiple_of(i * tile, tile), tile)
            v = dot3(xsh[r0, :], xsl[r0, :], yth[...], ytl[...])
            scores[r0, c0] = v
            v = v + start
            old = pm[r0, :]
            top = old
            for c in range(0, yb, 128):
                top = jnp.maximum(top, v[:, c:c + 128])
            acc = ps[r0, :] * jnp.exp2(old - top)
            for c in range(0, yb, 128):
                acc = acc + jnp.exp2(v[:, c:c + 128] - top)
            pm[r0, :] = top
            ps[r0, :] = acc
            return 0

        lax.fori_loop(0, rows // tile, body, 0)

    def blocks(d):
        lax.fori_loop(0, 2, lambda i, _: (block(at(d * (1 - 2 * i))), 0)[1], 0)

    for s in range(1, nr):
        ag_step(s)
        if s == nr // 2:
            peers_wait(nc, col, x_s, x_r, lambda k: x_full.at[k], in_col)
            lax.fori_loop(0, nc, prep_x, 0)
            lax.fori_loop(0, 2, lambda i, _: (block(at(i * s)), 0)[1], 0)
        elif s > nr // 2:
            blocks(s)

    rt = 32

    def row_pass(ph, keep):
        def body(i, _):
            r0 = pl.ds(pl.multiple_of(i * rt, rt), rt)
            top = scores[r0, 0:128] + gvec[:, 0:128]
            for c in range(128, cols, 128):
                top = jnp.maximum(top, scores[r0, c:c + 128] + gvec[:, c:c + 128])
            top = jnp.broadcast_to(jnp.max(top, axis=1, keepdims=True), (rt, 128))
            acc = jnp.zeros((rt, 128), jnp.float32)
            for c in range(0, cols, 128):
                e = jnp.exp2(scores[r0, c:c + 128] + gvec[:, c:c + 128] - top)
                acc = acc + e
                if keep:
                    eh[r0, c:c + 128], el[r0, c:c + 128] = split(e)
            pm[r0, :] = top
            ps[r0, :] = acc
            return 0

        lax.fori_loop(0, rows // rt, body, 0, unroll=2)
        row_send(ph)

    def row_send(ph):
        tops = pm[...].T
        top = jnp.max(tops, axis=0, keepdims=True)
        rstat[ph, col, 0:1, :] = top
        rstat[ph, col, 1:2, :] = jnp.sum(ps[...].T * jnp.exp2(tops - top), axis=0, keepdims=True)
        peers(nc, col, rst_s.at[ph], rst_r.at[ph], rstat.at[ph, col], rstat.at[ph, col], in_col)

    def merge(ref, n):
        peak = ref[0, 0:1, :]
        for k in range(1, n):
            peak = jnp.maximum(peak, ref[k, 0:1, :])
        total = ref[0, 1:2, :] * jnp.exp2(ref[0, 0:1, :] - peak)
        for k in range(1, n):
            total = total + ref[k, 1:2, :] * jnp.exp2(ref[k, 0:1, :] - peak)
        return peak, total

    def row_merge(ph):
        peers_wait(nc, col, rst_s.at[ph], rst_r.at[ph], lambda k: rstat.at[ph, k], in_col)
        return merge(rstat.at[ph], nc)

    def to_column(v):
        fcol[...] = jnp.broadcast_to(v, (128, rows)).T

    def col_pass(ph, keep):
        def body(i, _):
            c0 = pl.ds(pl.multiple_of(i * 128, 128), 128)
            a = scores[:, c0] + fcol[...]
            top = jnp.max(a, axis=0, keepdims=True)
            e = jnp.exp2(a - top)
            cstat[ph, row, 0:1, c0] = top
            cstat[ph, row, 1:2, c0] = jnp.sum(e, axis=0, keepdims=True)
            if keep:
                eh[:, c0], el[:, c0] = split(e)
            return 0

        lax.fori_loop(0, cols // 128, body, 0)
        peers(nr, row, cst_s.at[ph], cst_r.at[ph], cstat.at[ph, row], cstat.at[ph, row], in_row)

    def col_merge(ph):
        peers_wait(nr, row, cst_s.at[ph], cst_r.at[ph], lambda k: cstat.at[ph, k], in_row)
        return merge(cstat.at[ph], nr)

    for it in range(2):
        if it == 0:
            row_send(it)
        else:
            row_pass(it, False)
        peak, total = row_merge(it)
        f_new = -(peak + jnp.log2(total))
        if it == 1:
            f_ref[...] = f_new * BACK + xn[...]
        to_column(f_new)
        col_pass(it, it == 1)
        if it == 0:
            peak, total = col_merge(0)
            gvec[...] = -(peak + jnp.log2(total))

    def chunk(o):
        return pl.ds(pl.multiple_of(o * yb, yb), yb)

    def weigh(s, d):
        c0 = chunk(at(-sides[d] * (1 + s)))
        w0 = pl.ds(d * hw, hw)
        part[w0, c0] = dot3(xth[w0, :], xtl[w0, :], eh[:, c0], el[:, c0])

    def weigh_steps(lo, hi):
        def body(s, _):
            for d in range(2):
                weigh(s, d)
            return 0

        lax.fori_loop(lo, hi, body, 0)

    def rs_step(s):
        for q in range(PIECES):
            for d in range(2):
                c0 = chunk(at(-sides[d] * (1 + s)))
                own = part[pl.ds(d * hw + q * hq, hq), c0] * cloc[:, c0]
                cut, dev = pl.ds(q * hq, hq), (at(sides[d]), col)
                if s == 0:
                    src = first.at[d, cut]
                    first[d, cut] = own
                else:
                    src = rsbuf.at[s - 1, d, cut]
                    arrive(src, rs_s.at[s - 1, d, q], rs_r.at[s - 1, d, q], dev)
                    own = rsbuf[s - 1, d, cut] + own
                    if s < nr - 1:
                        rsbuf[s - 1, d, cut] = own
                if s < nr - 1:
                    send(src, rsbuf.at[s, d, cut], rs_s.at[s, d, q], rs_r.at[s, d, q], dev)
                else:
                    w0 = d * hw + q * hq
                    dt_ref[:, w0:w0 + hq] = own.T

    weigh_steps(0, nr // 2)
    peak, total = col_merge(1)
    cloc[...] = jnp.exp2(cstat[1, row, 0:1, :] - peak) / total * (1.0 / SCALE)
    rs_step(0)
    gvec[...] = -(peak + jnp.log2(total))
    g_ref[...] = gvec[...] * BACK + yn[...]
    weigh_steps(nr // 2, nr)
    rs_step(1)

    row_pass(2, True)
    rs_step(2)

    def spread(k):
        r0 = pl.ds(pl.multiple_of(k * xb, xb), xb)
        npart[r0, :] = dot3(eh[r0, :], el[r0, :], ysh[...], ysl[...])

    mid = max(1, nc // 2)
    lax.fori_loop(0, mid, lambda i, _: (spread(lax.rem(col + 1 + i, nc)), 0)[1], 0)
    peak, total = row_merge(2)
    to_column(jnp.exp2(rstat[2, col, 0:1, :] - peak) / total)

    def scaled(k):
        r0 = pl.ds(pl.multiple_of(k * xb, xb), xb)
        fc = fcol[r0, :]
        for c in range(0, w, 128):
            npart[r0, c:c + 128] = npart[r0, c:c + 128] * fc
        return r0

    def push(o):
        k = lax.rem(col + o, nc)
        r0 = scaled(k)
        send(npart.at[r0], nsbuf.at[col], ns_s.at[o], ns_r.at[col], in_col(k))

    for o in range(1, min(mid + 1, nc)):
        push(o)
    if nr > 4:
        rs_step(3)
    lax.fori_loop(mid, nc, lambda i, _: (spread(lax.rem(col + 1 + i, nc)), 0)[1], 0)
    for o in range(mid + 1, nc):
        push(o)
    nsbuf[col] = npart[scaled(col), :]
    for s in range(4 if nr > 4 else 3, nr - 1):
        rs_step(s)
    peers_wait(nc, col, ns_s, ns_r, lambda k: nsbuf.at[k], in_col)
    acc = nsbuf[0]
    for k in range(1, nc):
        acc = acc + nsbuf[k]
    nt_ref[...] = acc
    rs_step(nr - 1)
    for c in pending:
        c.wait_send()


def solution(mesh):
    nr, nc = mesh.shape["row"], mesh.shape["col"]

    def shards(noise, data):
        xb, w = noise.shape
        yb = data.shape[0]
        rows, cols = xb * nc, yb * nr
        f32, bf = jnp.float32, jnp.bfloat16
        vmem = pltpu.VMEM
        dma = pltpu.SemaphoreType.DMA
        out = pl.pallas_call(
            functools.partial(kernel, nr, nc),
            out_shape=(
                jax.ShapeDtypeStruct((xb, w), f32),
                jax.ShapeDtypeStruct((yb, w), f32),
                jax.ShapeDtypeStruct((1, rows), f32),
                jax.ShapeDtypeStruct((1, cols), f32),
            ),
            in_specs=[pl.BlockSpec(memory_space=pltpu.VMEM)] * 2,
            out_specs=(pl.BlockSpec(memory_space=pltpu.VMEM),) * 4,
            scratch_shapes=[
                vmem((nc, xb, w), f32), vmem((nr, yb, w), f32), vmem((rows, cols), f32),
                vmem((rows, w), bf), vmem((rows, w), bf), vmem((w, rows), bf), vmem((w, rows), bf),
                vmem((cols, w), bf), vmem((cols, w), bf), vmem((w, yb), bf), vmem((w, yb), bf),
                vmem((rows, cols), bf), vmem((rows, cols), bf), vmem((w, cols), f32), vmem((rows, w), f32),
                vmem((rows, 128), f32), vmem((rows, 128), f32), vmem((rows, 128), f32),
                vmem((1, rows), f32), vmem((1, cols), f32), vmem((1, cols), f32), vmem((1, cols), f32),
                vmem((3, nc, 2, rows), f32), vmem((2, nr, 2, cols), f32),
                vmem((nr - 1, 2, w // 2, yb), f32), vmem((2, w // 2, yb), f32), vmem((nc, xb, w), f32),
                dma((nr - 1, 2, PIECES)), dma((nr - 1, 2, PIECES)), dma((nc,)), dma((nc,)),
                dma((3, nc)), dma((3, nc)), dma((2, nr)), dma((2, nr)),
                dma((nr - 1, 2, PIECES)), dma((nr - 1, 2, PIECES)), dma((nc,)), dma((nc,)),
            ],
            compiler_params=pltpu.CompilerParams(
                collective_id=0, has_side_effects=True, vmem_limit_bytes=60 * 1024 * 1024
            ),
        )(noise, data)
        return out[0], out[1], out[2].reshape(rows), out[3].reshape(cols)

    return jax.shard_map(
        shards,
        mesh=mesh,
        in_specs=(P(("row", "col"), None), P(("col", "row"), None)),
        out_specs=(P(("row", "col"), None), P(("col", "row"), None), P("row"), P("col")),
        check_vma=False,
    )
```
